32 devices in a mesh: dp: 8 (over z, x), tensor: 4 (over y, core).
Axes of the slice: x: 2, y: 2, z: 4, core: 2. Of those that a mesh axis runs over, the one named last changes fastest.
Arguments:
- hidden: bfloat16 [8192, 2560], P('dp', 'tensor'), may hold values from -6 to 6
- out_grad: bfloat16 [8192, 2560], P('dp', 'tensor'), may hold values from -6 to 6
- memory: bfloat16 [8192, 1280], P('dp'), may hold values from -6 to 6
- w_key: bfloat16 [1280, 2560], P(None, 'tensor'), may hold values from -0.15625 to 0.15625
- w_value: bfloat16 [1280, 2560], P(None, 'tensor'), may hold values from -0.15625 to 0.15625
- row_owner: int32 [8192, 8], P('dp'), may hold values from 0 to 31, all different within a row; in each aligned block of 256 rows (0 to 255, 256 to 511, ...) at most 128 rows name the same one
- row_slot: int32 [8192, 8], P('dp'), may hold values from 0 to 511
- mem_table: float32 [16384, 160], P(('dp', 'tensor')), may hold values from -6 to 6
- adagrad_sum: float32 [16384, 160], P(('dp', 'tensor')), may hold values from 0.05 to 2
Outputs:
- hidden_grad: bfloat16 [8192, 2560], P('dp', 'tensor')
- key_weight_grad: float32 [1280, 2560], P('dp', 'tensor')
- value_weight_grad: float32 [1280, 2560], P('dp', 'tensor')
- new_table: float32 [16384, 160], P(('dp', 'tensor'))
- new_sum: float32 [16384, 160], P(('dp', 'tensor'))
The draws below stay inside these ranges and needn't reach their ends.
Inputs may be any that keep to these rules, and one draw needn't show every extreme that they name: `row_owner`: each token's 8 owners are distinct. Within a dp shard, take the tokens in order in aligned blocks of 256: in each block no owner is named more than 128 times, a bound that some owner reaches in some or all blocks. `row_slot`: A few row indices are retrieved very often.
All inputs are finite; a program needn't handle non-finite values.
Results may differ from the reference program's by a relative error of at most 0.0034.
Values sent between devices are 32-bit elements; how exact they have to be, the bound alone decides.
A program may use at most 128 MiB of HBM per device.

```python
import math
import jax
import jax.numpy as jnp
import numpy as np
from jax import lax

D = 2560
ME = 1280
H = 8
TOK_DEV = 1024
R_DEV = 512
CAP = 128
EH = 160
TOKENS = 8192
ROWS = 16384
N_DP = 8
N_TENSOR = 4


def touch_ends(entries, stream_key, least, high):
    extent = entries.shape
    index_at = [jax.random.randint(jax.random.fold_in(stream_key, axis), (), 0, extent[axis]) for axis in range(len(extent))]
    entries = entries.at[tuple(index_at)].set(least)
    longest = extent.index(max(extent))
    index_at[longest] = (index_at[longest] + 1) % extent[longest]
    return entries.at[tuple(index_at)].set(high)


def block_scale(rng, dims, pieces, smallest, high):
    gain = 1.0
    for position, parts in pieces:
        steps = jax.random.uniform(jax.random.fold_in(jax.random.fold_in(rng, 6), position), (parts,), jnp.float32, smallest / len(pieces), high / len(pieces))
        gain = gain * jnp.repeat(jnp.exp(steps), dims[position] // parts).reshape((-1,) + (1,) * (len(dims) - 1 - position))
    return gain


def cumulative_ranks(number_of, lean):
    loads = [(1 << 20) // math.isqrt(rank ** lean) + 1 for rank in range(1, number_of + 1)]
    scale = 1 + sum(loads) // (1 << 30)
    return np.cumsum(np.array([max(1, weight // scale) for weight in loads]))


def ranked_ids(own_key, shape, amount, skew):
    table = cumulative_ranks(amount, skew)
    ticket = jax.random.randint(jax.random.fold_in(own_key, 1), shape, 0, int(table[amount - 1]))
    grade = jnp.searchsorted(jnp.asarray(table, jnp.int32), ticket, side="right")
    return jax.random.permutation(jax.random.fold_in(own_key, 2), amount)[grade].astype(jnp.int32)


def assign_block(key, own, number, rows, number_of, top, reach, skew):
    sequence = jax.random.permutation(key, number_of)
    crowded, ordinary = portions_of(number_of, rows * top, reach, skew, True), portions_of(number_of, rows * top, reach, skew, False)
    places = jnp.arange(number_of)

    def named(tallies, rotation):
        used = int((tallies > 0).sum())
        fixed = max(1, used // 4)
        passed = fixed + (places - fixed + rotation * (used - fixed)) % max(1, number_of - fixed)
        return jnp.zeros((number_of,), jnp.int32).at[sequence[jnp.where(places < fixed, places, passed)]].set(jnp.asarray(tallies, jnp.int32))

    tallies = jnp.where(number % 4 == 0, named(crowded, number // 4), named(ordinary, number - number // 4 - 1))
    mixed = jax.random.permutation(jax.random.fold_in(own, 3), number_of)
    donor, receiver = mixed[0:number_of // 2 * 2:2], mixed[1:number_of // 2 * 2:2]
    margin = jnp.minimum(tallies[donor] - 1, reach - tallies[receiver]) // 2
    margin = jnp.where((donor == sequence[0]) | (receiver == sequence[0]) | (tallies[receiver] == 0), 0, jnp.maximum(margin, 0))
    passed = jax.random.randint(jax.random.fold_in(own, 4), (number_of // 2,), 0, 1 << 20) % (margin + 1)
    tallies = tallies.at[donor].add(-passed).at[receiver].add(passed)
    members = jnp.searchsorted(jnp.cumsum(tallies), jnp.arange(rows * top), side="right").astype(jnp.int32)
    table = members.reshape(top, rows).T
    table = table[jax.random.permutation(jax.random.fold_in(own, 1), rows)]
    rotation = jax.random.randint(jax.random.fold_in(own, 2), (rows, 1), 0, top)
    return jnp.take_along_axis(table, (jnp.arange(top)[None, :] + rotation) % top, axis=1)


def portions_of(number_of, total, bound, slope, full):
    portions = [(1 << 20) // math.isqrt(grade ** slope) + 1 for grade in range(1, number_of + 1)]
    largest = bound if full else min(bound, max(-(-total // number_of), total * portions[0] // sum(portions)))
    least = 1 if total - largest >= number_of - 1 else 0
    given, spare = [largest] + [least] * (number_of - 1), total - largest - least * (number_of - 1)
    while spare > 0:
        candidates = [i for i in range(1, number_of) if given[i] < largest] or [i for i in range(1, number_of) if given[i] < bound]
        mass, remaining = sum([portions[i] for i in candidates]), spare
        for i in candidates:
            extra = min(bound - given[i], max(1, remaining * portions[i] // mass), spare)
            given[i] = given[i] + extra
            spare = spare - extra
    return np.array(given)


def noise(key, extent, deviation, reach, shards=(), dtype=jnp.bfloat16):
    values = jax.random.normal(key, extent, jnp.float32) * deviation
    if len(shards) > 0:
        values = block_scale(key, extent, shards, -0.22, 0.18) * values
    return jnp.clip(values, min=-reach, max=reach).astype(dtype)


def setup_inputs(seed: int = 0) -> dict:
    streams_of = jax.random.split(jax.random.key(seed), 10)
    hidden = noise(streams_of[0], (TOKENS, D), 1.0, 6.0, ((0, 8), (1, 4)))
    out_grad = noise(streams_of[1], (TOKENS, D), 1.0, 6.0, ((0, 8), (1, 4)))
    memory = noise(streams_of[2], (TOKENS, ME), 1.0, 6.0, ((0, 8),))
    w_key = noise(streams_of[3], (ME, D), ME ** -0.5, 0.15625, ((1, 4),))
    w_value = noise(streams_of[4], (ME, D), ME ** -0.5, 0.15625, ((1, 4),))
    row_owner_keys = jax.random.split(jax.random.fold_in(streams_of[5], 1), TOKENS // (TOK_DEV // N_TENSOR))
    row_owner_turns = jax.random.permutation(jax.random.fold_in(streams_of[5], 3), TOKENS // (TOK_DEV // N_TENSOR))
    row_owner = jax.vmap(lambda own, number: assign_block(jax.random.fold_in(streams_of[5], 2), own, number, TOK_DEV // N_TENSOR, N_DP * N_TENSOR, H, CAP, 2))(row_owner_keys, row_owner_turns).reshape((TOKENS, H))
    row_slot = touch_ends(ranked_ids(streams_of[6], (TOKENS, H), R_DEV, 2), jax.random.fold_in(streams_of[6], 3), 0, R_DEV - 1).astype(jnp.int32)
    mem_table = noise(streams_of[7], (ROWS, EH), 1.0, 6.0, ((0, 32),), jnp.float32)
    adagrad_sum = jnp.clip(jnp.exp(math.log(2.0) - 3.6888794 * jax.random.uniform(streams_of[8], (ROWS, EH), jnp.float32) ** block_scale(streams_of[8], (ROWS, EH), ((0, 32),), -0.2, 0.2)), 0.05, 2.0)
    return {"hidden": hidden, "out_grad": out_grad, "memory": memory, "w_key": w_key, "w_value": w_value, "row_owner": row_owner, "row_slot": row_slot, "mem_table": mem_table, "adagrad_sum": adagrad_sum}


LEARN_RATE = 0.5
EPSILON = 1e-06

def reference(hidden, out_grad, memory, w_key, w_value, row_owner, row_slot, mem_table, adagrad_sum):
    scale_root = jnp.sqrt(jnp.asarray(D, jnp.float32))
    proj_key = jnp.dot(memory, w_key, preferred_element_type=jnp.float32)
    proj_value = jnp.dot(memory, w_value, preferred_element_type=jnp.float32)
    scores = lax.optimization_barrier(jnp.sum(hidden.astype(jnp.float32) * proj_key, axis=1)) / scale_root
    gate_value = jax.nn.sigmoid(scores)
    gate_grad = lax.optimization_barrier(jnp.sum(out_grad.astype(jnp.float32) * proj_value, axis=1))
    score_grad = gate_grad * gate_value * (1.0 - gate_value) / scale_root
    value_grad = (gate_value[:, None] * out_grad.astype(jnp.float32)).astype(jnp.bfloat16)
    key_grad = (score_grad[:, None] * hidden.astype(jnp.float32)).astype(jnp.bfloat16)
    hidden_grad = (score_grad[:, None] * proj_key).astype(jnp.bfloat16)
    over_tokens = (((0,), (0,)), ((), ()))
    key_weight_grad = lax.dot_general(memory, key_grad, over_tokens, preferred_element_type=jnp.float32)
    value_weight_grad = lax.dot_general(memory, value_grad, over_tokens, preferred_element_type=jnp.float32)
    over_features = (((1,), (1,)), ((), ()))
    memory_grad = lax.dot_general(value_grad, w_value, over_features, preferred_element_type=jnp.float32)
    memory_grad = memory_grad + lax.dot_general(key_grad, w_key, over_features, preferred_element_type=jnp.float32)
    row_index = (row_owner * R_DEV + row_slot).reshape(-1).astype(jnp.int32)
    row_grads = memory_grad.reshape(-1, ME // H)
    row_sum = jax.ops.segment_sum(row_grads, row_index, num_segments=R_DEV * N_DP * N_TENSOR)
    new_sum = adagrad_sum + row_sum * row_sum
    new_table = mem_table - LEARN_RATE * row_sum / (jnp.sqrt(new_sum) + EPSILON)
    return (hidden_grad, key_weight_grad, value_weight_grad, new_table, new_sum)
```

```python
import functools

import jax
import jax.numpy as jnp
from jax import lax
from jax.experimental import pallas as pl
from jax.experimental.pallas import tpu as pltpu
from jax.sharding import PartitionSpec as P

LEARN_RATE = 0.5
EPSILON = 1e-06
MESH = pl.DeviceIdType.MESH
OVER_FEATURES = (((1,), (1,)), ((), ()))


def gate_kernel(count, part_ref, sum_ref, landed, send_sem, recv_sem):
    me = lax.axis_index("tensor")
    dp = lax.axis_index("dp")
    barrier = pltpu.get_barrier_semaphore()
    for k in range(1, count):
        pl.semaphore_signal(
            barrier, inc=1, device_id=(dp, lax.rem(me + k, count)), device_id_type=MESH
        )
    pl.semaphore_wait(barrier, count - 1)
    copies = []
    for k in range(1, count):
        copy = pltpu.make_async_remote_copy(
            src_ref=part_ref,
            dst_ref=landed.at[me],
            send_sem=send_sem.at[k],
            recv_sem=recv_sem.at[k],
            device_id=(dp, lax.rem(me + k, count)),
            device_id_type=MESH,
        )
        copy.start()
        copies.append(copy)
    landed[me] = part_ref[...]
    for copy in copies:
        copy.wait()
    total = landed[0]
    for k in range(1, count):
        total = total + landed[k]
    sum_ref[...] = total


def sum_over_tensor(parts, count):
    return pl.pallas_call(
        functools.partial(gate_kernel, count),
        out_shape=jax.ShapeDtypeStruct(parts.shape, jnp.float32),
        in_specs=[pl.BlockSpec(memory_space=pltpu.VMEM)],
        out_specs=pl.BlockSpec(memory_space=pltpu.VMEM),
        scratch_shapes=[
            pltpu.VMEM((count,) + parts.shape, jnp.float32),
            pltpu.SemaphoreType.DMA((count,)),
            pltpu.SemaphoreType.DMA((count,)),
        ],
        compiler_params=pltpu.CompilerParams(collective_id=0, has_side_effects=True),
        name="gate_sum",
    )(parts)


def exchange_kernel(dp_count, tensor_count, send_ref, recv_ref, local_sem, send_sem, recv_sem):
    count = dp_count * tensor_count
    me = lax.axis_index("dp") * tensor_count + lax.axis_index("tensor")
    barrier = pltpu.get_barrier_semaphore()

    def target(k):
        other = lax.rem(me + k, count)
        return other, (lax.div(other, tensor_count), lax.rem(other, tensor_count))

    def greet(k, carry):
        pl.semaphore_signal(barrier, inc=1, device_id=target(k)[1], device_id_type=MESH)
        return carry

    lax.fori_loop(1, count, greet, 0)
    own = pltpu.make_async_copy(send_ref.at[me], recv_ref.at[me], local_sem)
    own.start()
    pl.semaphore_wait(barrier, count - 1)

    def copy_of(k):
        other, where = target(k)
        return pltpu.make_async_remote_copy(
            src_ref=send_ref.at[other],
            dst_ref=recv_ref.at[me],
            send_sem=send_sem.at[k],
            recv_sem=recv_sem.at[k],
            device_id=where,
            device_id_type=MESH,
        )

    def begin(k, carry):
        copy_of(k).start()
        return carry

    def finish(k, carry):
        copy_of(k).wait()
        return carry

    lax.fori_loop(1, count, begin, 0)
    own.wait()
    lax.fori_loop(1, count, finish, 0)


def exchange_rows(blocks, dp_count, tensor_count):
    count = dp_count * tensor_count
    return pl.pallas_call(
        functools.partial(exchange_kernel, dp_count, tensor_count),
        out_shape=jax.ShapeDtypeStruct(blocks.shape, jnp.float32),
        in_specs=[pl.BlockSpec(memory_space=pl.ANY)],
        out_specs=pl.BlockSpec(memory_space=pl.ANY),
        scratch_shapes=[
            pltpu.SemaphoreType.DMA,
            pltpu.SemaphoreType.DMA((count,)),
            pltpu.SemaphoreType.DMA((count,)),
        ],
        compiler_params=pltpu.CompilerParams(collective_id=1, has_side_effects=True),
        cost_estimate=pl.CostEstimate(
            flops=50_000_000_000, bytes_accessed=2 * blocks.size * 4, transcendentals=0
        ),
        name="exchange_rows",
    )(blocks)


def halves(values):
    high = values.astype(jnp.bfloat16)
    return high, (values - high.astype(jnp.float32)).astype(jnp.bfloat16)


def pack_kernel(width, grads_ref, owners_ref, slots_ref, places_ref, out_ref):
    heads, tokens = owners_ref.shape
    count, capacity = out_ref.shape[0], out_ref.shape[2]
    group = 2

    def step(i, carry):
        for j in range(group):
            dest = i * group + j
            mask = owners_ref[...] == dest
            rows = jnp.zeros((width, tokens), jnp.float32)
            for h in range(heads):
                rows = jnp.where(mask[h : h + 1, :], grads_ref[h * width : (h + 1) * width, :], rows)
            tags = jnp.where(mask, slots_ref[...] + 1.0, 0.0)
            place = places_ref[pl.ds(dest, 1), :]
            spots = lax.broadcasted_iota(jnp.int32, (capacity, tokens), 0)
            choose = (spots == place).astype(jnp.float32).astype(jnp.bfloat16)
            for values, first, last in ((rows, 0, width), (tags, width, width + heads)):
                high, low = halves(values)
                out_ref[dest, first:last, :] = lax.dot_general(
                    high, choose, OVER_FEATURES, preferred_element_type=jnp.float32
                ) + lax.dot_general(low, choose, OVER_FEATURES, preferred_element_type=jnp.float32)
        return carry

    lax.fori_loop(0, count // group, step, 0)


def pack_rows(grads, owners, slots, places, capacity):
    heads, count = owners.shape[0], places.shape[0]
    width = grads.shape[0] // heads
    return pl.pallas_call(
        functools.partial(pack_kernel, width),
        out_shape=jax.ShapeDtypeStruct((count, width + heads, capacity), jnp.float32),
        in_specs=[pl.BlockSpec(memory_space=pltpu.VMEM)] * 4,
        out_specs=pl.BlockSpec(memory_space=pltpu.VMEM),
        cost_estimate=pl.CostEstimate(
            flops=6_000_000_000, bytes_accessed=4_000_000, transcendentals=0
        ),
        name="pack_rows",
    )(grads, owners, slots, places)


def update_kernel(group, recv_ref, table_ref, sums_ref, new_table_ref, new_sums_ref, total):
    rows, width = table_ref.shape
    count, _, capacity = recv_ref.shape
    total[...] = jnp.zeros_like(total)

    def step(i, carry):
        picks, highs, lows = [], [], []
        for j in range(group):
            block = recv_ref[i * group + j]
            tag = jnp.sum(block[width:, :], axis=0, keepdims=True).astype(jnp.int32) - 1
            ids = lax.broadcasted_iota(jnp.int32, (rows, capacity), 0)
            picks.append((ids == tag).astype(jnp.float32).astype(jnp.bfloat16))
            high, low = halves(block[:width, :])
            highs.append(high)
            lows.append(low)
        pick = jnp.concatenate(picks, axis=1) if group > 1 else picks[0]
        high = jnp.concatenate(highs, axis=1) if group > 1 else highs[0]
        low = jnp.concatenate(lows, axis=1) if group > 1 else lows[0]
        total[...] += lax.dot_general(
            pick, high, OVER_FEATURES, preferred_element_type=jnp.float32
        ) + lax.dot_general(pick, low, OVER_FEATURES, preferred_element_type=jnp.float32)
        return carry

    lax.fori_loop(0, count // group, step, 0)
    row_sum = total[...]
    new_sum = sums_ref[...] + row_sum * row_sum
    new_sums_ref[...] = new_sum
    new_table_ref[...] = table_ref[...] - LEARN_RATE * row_sum / (jnp.sqrt(new_sum) + EPSILON)


def update_rows(recv, table, sums):
    group = 4 if recv.shape[2] % 128 == 0 and recv.shape[0] % 4 == 0 else 1
    return pl.pallas_call(
        functools.partial(update_kernel, group),
        out_shape=(jax.ShapeDtypeStruct(table.shape, jnp.float32),) * 2,
        in_specs=[pl.BlockSpec(memory_space=pltpu.VMEM)] * 3,
        out_specs=(pl.BlockSpec(memory_space=pltpu.VMEM),) * 2,
        scratch_shapes=[pltpu.VMEM(table.shape, jnp.float32)],
        cost_estimate=pl.CostEstimate(
            flops=6_000_000_000, bytes_accessed=5_000_000, transcendentals=0
        ),
        name="update_rows",
    )(recv, table, sums)


def swap(values, axis, bit):
    count = lax.axis_size(axis)
    return lax.ppermute(values, axis, [(i, i ^ (1 << bit)) for i in range(count)])


def scatter_sum(values, order):
    count = lax.axis_size("dp")
    bits = count.bit_length() - 1
    me = lax.axis_index("dp")
    left = list(range(bits))[::-1]
    values = values.reshape((2,) * bits + (values.shape[0] // count, values.shape[1]))
    for bit in order:
        axis = left.index(bit)
        mine = lax.rem(lax.div(me, 1 << bit), 2)
        sent = lax.dynamic_index_in_dim(values, 1 - mine, axis, keepdims=False)
        kept = lax.dynamic_index_in_dim(values, mine, axis, keepdims=False)
        values = kept + swap(sent, "dp", bit)
        left.remove(bit)
    return values


def body(hidden, out_grad, memory, w_key, w_value, row_owner, row_slot, mem_table, adagrad_sum):
    dp_count, tensor_count = lax.axis_size("dp"), lax.axis_size("tensor")
    owner_count = dp_count * tensor_count
    tokens = memory.shape[0]
    quarter = tokens // tensor_count
    features = w_key.shape[1] * tensor_count
    heads = row_owner.shape[1]
    scale_root = jnp.sqrt(jnp.asarray(features, jnp.float32))
    me = lax.axis_index("tensor")

    spread = tensor_count.bit_length() - 1
    firsts, extent = [], tokens
    for bit in range(spread):
        extent //= 2
        firsts.append(lax.rem(lax.div(me, 1 << bit), 2))
    first_row, extent = 0, tokens
    for mine in firsts:
        extent //= 2
        first_row = first_row + mine * extent
    owners = lax.dynamic_slice_in_dim(row_owner, first_row, quarter, 0).T
    slots = lax.dynamic_slice_in_dim(row_slot, first_row, quarter, 0).T.astype(jnp.float32)
    owner_ids = jnp.arange(owner_count, dtype=jnp.int32)
    hits = jnp.any(owners[None, :, :] == owner_ids[:, None, None], axis=1)
    token_ids = jnp.arange(quarter, dtype=jnp.int32)
    earlier = (token_ids[:, None] < token_ids[None, :]).astype(jnp.bfloat16)
    before = jnp.dot(hits.astype(jnp.bfloat16), earlier, preferred_element_type=jnp.float32)
    places = jnp.where(hits, before.astype(jnp.int32), -1)
    capacity = max(2, 2 * quarter * heads // owner_count)

    proj_key = jnp.dot(memory, w_key, preferred_element_type=jnp.float32)
    proj_value = jnp.dot(memory, w_value, preferred_element_type=jnp.float32)
    part_score = jnp.sum(hidden.astype(jnp.float32) * proj_key, axis=1)
    part_gate = jnp.sum(out_grad.astype(jnp.float32) * proj_value, axis=1)
    parts = jnp.stack([part_score, part_gate]).reshape(2, tokens // 128, 128)
    scores, gate_grad = sum_over_tensor(parts, tensor_count).reshape(2, tokens)
    gate_value = jax.nn.sigmoid(scores / scale_root)
    score_grad = gate_grad * gate_value * (1.0 - gate_value) / scale_root
    value_grad = (gate_value[:, None] * out_grad.astype(jnp.float32)).astype(jnp.bfloat16)
    key_grad = (score_grad[:, None] * hidden.astype(jnp.float32)).astype(jnp.bfloat16)
    hidden_grad = (score_grad[:, None] * proj_key).astype(jnp.bfloat16)

    def memory_grad_of(first, extent):
        value_part = lax.dynamic_slice_in_dim(value_grad, first, extent, 0)
        key_part = lax.dynamic_slice_in_dim(key_grad, first, extent, 0)
        return lax.dot_general(
            w_value, value_part, OVER_FEATURES, preferred_element_type=jnp.float32
        ) + lax.dot_general(w_key, key_part, OVER_FEATURES, preferred_element_type=jnp.float32)

    half = tokens // 2
    sent = memory_grad_of((1 - firsts[0]) * half, half)
    landed = swap(sent, "tensor", 0)
    memory_grad = memory_grad_of(firsts[0] * half, half) + landed
    for bit in range(1, spread):
        half //= 2
        sent = lax.dynamic_slice_in_dim(memory_grad, (1 - firsts[bit]) * half, half, 1)
        kept = lax.dynamic_slice_in_dim(memory_grad, firsts[bit] * half, half, 1)
        memory_grad = kept + swap(sent, "tensor", bit)

    over_tokens = (((0,), (0,)), ((), ()))
    key_total = lax.dot_general(memory, key_grad, over_tokens, preferred_element_type=jnp.float32)
    value_total = lax.dot_general(
        memory, value_grad, over_tokens, preferred_element_type=jnp.float32
    )
    order = list(range(dp_count.bit_length() - 1))
    other_order = order[1:2] + order[:1] + order[2:]
    key_weight_grad = scatter_sum(key_total, order)
    value_weight_grad = scatter_sum(value_total, other_order)

    packed = pack_rows(memory_grad, owners, slots, places, capacity)
    recv = exchange_rows(packed, dp_count, tensor_count)
    new_table, new_sum = update_rows(recv, mem_table, adagrad_sum)
    return (hidden_grad, key_weight_grad, value_weight_grad, new_table, new_sum)


def solution(mesh):
    return jax.shard_map(
        body,
        mesh=mesh,
        in_specs=(
            P("dp", "tensor"),
            P("dp", "tensor"),
            P("dp", None),
            P(None, "tensor"),
            P(None, "tensor"),
            P("dp", None),
            P("dp", None),
            P(("dp", "tensor"), None),
            P(("dp", "tensor"), None),
        ),
        out_specs=(
            P("dp", "tensor"),
            P("dp", "tensor"),
            P("dp", "tensor"),
            P(("dp", "tensor"), None),
            P(("dp", "tensor"), None),
        ),
        check_vma=False,
    )
```

```python
import functools

import jax
import jax.numpy as jnp
from jax import lax
from jax.experimental import pallas as pl
from jax.experimental.pallas import tpu as pltpu
from jax.sharding import PartitionSpec as P

LEARN_RATE = 0.5
EPSILON = 1e-06
MESH = pl.DeviceIdType.MESH
OVER_FEATURES = (((1,), (1,)), ((), ()))


def gate_kernel(count, part_ref, sum_ref, landed, send_sem, recv_sem):
    me = lax.axis_index("tensor")
    dp = lax.axis_index("dp")
    barrier = pltpu.get_barrier_semaphore()
    for k in range(1, count):
        pl.semaphore_signal(
            barrier, inc=1, device_id=(dp, lax.rem(me + k, count)), device_id_type=MESH
        )
    pl.semaphore_wait(barrier, count - 1)
    copies = []
    for k in range(1, count):
        copy = pltpu.make_async_remote_copy(
            src_ref=part_ref,
            dst_ref=landed.at[me],
            send_sem=send_sem.at[k],
            recv_sem=recv_sem.at[k],
            device_id=(dp, lax.rem(me + k, count)),
            device_id_type=MESH,
        )
        copy.start()
        copies.append(copy)
    landed[me] = part_ref[...]
    for copy in copies:
        copy.wait()
    total = landed[0]
    for k in range(1, count):
        total = total + landed[k]
    sum_ref[...] = total


def sum_over_tensor(parts, count):
    return pl.pallas_call(
        functools.partial(gate_kernel, count),
        out_shape=jax.ShapeDtypeStruct(parts.shape, jnp.float32),
        in_specs=[pl.BlockSpec(memory_space=pltpu.VMEM)],
        out_specs=pl.BlockSpec(memory_space=pltpu.VMEM),
        scratch_shapes=[
            pltpu.VMEM((count,) + parts.shape, jnp.float32),
            pltpu.SemaphoreType.DMA((count,)),
            pltpu.SemaphoreType.DMA((count,)),
        ],
        compiler_params=pltpu.CompilerParams(collective_id=0, has_side_effects=True),
        name="gate_sum",
    )(parts)


def halves(values):
    high = values.astype(jnp.bfloat16)
    return high, (values - high.astype(jnp.float32)).astype(jnp.bfloat16)


def pack(width, grads_ref, owners_ref, slots_ref, places_ref, out_ref):
    heads, tokens = owners_ref.shape
    count, capacity = out_ref.shape[0], out_ref.shape[2]
    group = 2

    def step(i, carry):
        for j in range(group):
            dest = i * group + j
            mask = owners_ref[...] == dest
            rows = jnp.zeros((width, tokens), jnp.float32)
            for h in range(heads):
                rows = jnp.where(mask[h : h + 1, :], grads_ref[h * width : (h + 1) * width, :], rows)
            tags = jnp.where(mask, slots_ref[...] + 1.0, 0.0)
            place = places_ref[pl.ds(dest, 1), :]
            spots = lax.broadcasted_iota(jnp.int32, (capacity, tokens), 0)
            choose = (spots == place).astype(jnp.float32).astype(jnp.bfloat16)
            for values, first, last in ((rows, 0, width), (tags, width, width + heads)):
                high, low = halves(values)
                out_ref[dest, first:last, :] = lax.dot_general(
                    high, choose, OVER_FEATURES, preferred_element_type=jnp.float32
                ) + lax.dot_general(low, choose, OVER_FEATURES, preferred_element_type=jnp.float32)
        return carry

    lax.fori_loop(0, count // group, step, 0)


def fabric_kernel(
    dp_count, tensor_count, width, sent_ref, kept_ref, key_ref, value_ref, owners_ref, slots_ref,
    places_ref, recv_ref, key_out_ref, value_out_ref, *scratch
):
    count = dp_count * tensor_count
    stages, spread = dp_count.bit_length() - 1, tensor_count.bit_length() - 1
    refs = list(scratch)
    grads, kept, blocks, own = refs[:4]
    del refs[:4]
    lands, refs = refs[:stages], refs[stages:]
    parts, refs = refs[:stages], refs[stages:]
    grad_lands, refs = refs[:spread], refs[spread:]
    grad_sends, refs = refs[: spread - 1], refs[spread - 1 :]
    (local_sem, wsend_sem, wrecv_sem, gsend_sem, grecv_sem, send_sem, recv_sem) = refs
    dp, tensor = lax.axis_index("dp"), lax.axis_index("tensor")
    me = dp * tensor_count + tensor
    dp_bits = [lax.rem(lax.div(dp, 1 << s), 2) for s in range(stages)]
    bits = [lax.rem(lax.div(tensor, 1 << s), 2) for s in range(spread)]
    started = []
    weights = (key_ref, value_ref)

    def target(k):
        other = lax.rem(me + k, count)
        return other, (lax.div(other, tensor_count), lax.rem(other, tensor_count))

    barrier = pltpu.get_barrier_semaphore()

    def greet(k, carry):
        pl.semaphore_signal(barrier, inc=1, device_id=target(k)[1], device_id_type=MESH)
        return carry

    lax.fori_loop(1, count, greet, 0)
    locals_ = [pltpu.make_async_copy(kept_ref, kept, local_sem.at[0])]
    for w in range(2):
        locals_.append(
            pltpu.make_async_copy(weights[w].at[:, dp_bits[0]], own.at[w], local_sem.at[1 + w])
        )
    for copy in locals_:
        copy.start()
    pl.semaphore_wait(barrier, count - 1)

    height = kept.shape[0]
    chunks = 4
    chunk = height // chunks

    def grad_copy(source, bit, c):
        rows = pl.ds(c * chunk, chunk)
        return pltpu.make_async_remote_copy(
            src_ref=source.at[rows],
            dst_ref=grad_lands[bit].at[rows],
            send_sem=gsend_sem.at[bit, c],
            recv_sem=grecv_sem.at[bit, c],
            device_id=(dp, tensor + (1 - 2 * bits[bit]) * (1 << bit)),
            device_id_type=MESH,
        )

    grad_copies = [[grad_copy(sent_ref, 0, c) for c in range(chunks)]]
    for copy in grad_copies[0]:
        copy.start()

    def order(s):
        total = dp_count >> (s + 1)
        if total == 1:
            return [0], 0
        first = [2 * r + 1 - dp_bits[s + 1] for r in range(total // 2)]
        return first + [2 * r + dp_bits[s + 1] for r in range(total // 2)], total // 2

    orders = [order(s) for s in range(stages)]
    weight_copies = {}

    def weight_send(s, p, w):
        q = orders[s][0][p]
        if s == 0:
            source = weights[w].at[q, 1 - dp_bits[0]]
        else:
            source = parts[s - 1].at[w, 2 * q + 1 - dp_bits[s]]
        copy = pltpu.make_async_remote_copy(
            src_ref=source,
            dst_ref=lands[s].at[w, q],
            send_sem=wsend_sem.at[s, p, w],
            recv_sem=wrecv_sem.at[s, p, w],
            device_id=(dp + (1 - 2 * dp_bits[s]) * (1 << s), tensor),
            device_id_type=MESH,
        )
        copy.start()
        weight_copies[s, p, w] = copy

    def weight_add(s, p, w):
        q = orders[s][0][p]
        weight_copies[s, p, w].wait_recv()
        before = own[w, q] if s == 0 else parts[s - 1][w, 2 * q + dp_bits[s]]
        parts[s][w, q] = before + lands[s][w, q]

    for p in range(len(orders[0][0])):
        for w in range(2):
            weight_send(0, p, w)
    for copy in locals_:
        copy.wait()

    extent = kept.shape[1] // 2

    def columns(bit, kept_one):
        first = bits[bit] if kept_one else 1 - bits[bit]
        return pl.ds(pl.multiple_of(first * extent, 128 if extent % 128 == 0 else extent), extent)

    assert spread == 2
    forwarded = []
    for c in range(chunks):
        rows = pl.ds(c * chunk, chunk)
        grad_copies[0][c].wait_recv()
        away, here = columns(1, False), columns(1, True)
        grad_sends[0][rows] = kept[rows, away] + grad_lands[0][rows, away]
        copy = grad_copy(grad_sends[0], 1, c)
        copy.start()
        forwarded.append(copy)
        grads[rows] = kept[rows, here] + grad_lands[0][rows, here]
    grad_copies.append(forwarded)

    def first_half(s):
        for p in range(orders[s][1]):
            for w in range(2):
                weight_add(s, p, w)

    first_half(0)
    if stages > 1:
        for p in range(len(orders[1][0])):
            for w in range(2):
                weight_send(1, p, w)
    for c in range(chunks):
        rows = pl.ds(c * chunk, chunk)
        forwarded[c].wait_recv()
        grads[rows] = grads[rows] + grad_lands[1][rows]

    pack(width, grads, owners_ref, slots_ref, places_ref, blocks)

    kept_block = pltpu.make_async_copy(blocks.at[me], recv_ref.at[me], local_sem.at[3])
    kept_block.start()

    def copy_of(k):
        other, where = target(k)
        return pltpu.make_async_remote_copy(
            src_ref=blocks.at[other],
            dst_ref=recv_ref.at[me],
            send_sem=send_sem.at[k],
            recv_sem=recv_sem.at[k],
            device_id=where,
            device_id_type=MESH,
        )

    def begin(k, carry):
        copy_of(k).start()
        return carry

    def finish(k, carry):
        copy_of(k).wait()
        return carry

    lax.fori_loop(1, count, begin, 0)

    for s in range(stages):
        for p in range(0 if s > 0 else orders[0][1], len(orders[s][0])):
            if s > 0 and p == orders[s][1] and s + 1 < stages:
                for p2 in range(len(orders[s + 1][0])):
                    for w in range(2):
                        weight_send(s + 1, p2, w)
            for w in range(2):
                weight_add(s, p, w)
    key_out_ref[...] = parts[stages - 1][0, 0]
    value_out_ref[...] = parts[stages - 1][1, 0]
    lax.fori_loop(1, count, finish, 0)
    kept_block.wait()
    for copy in weight_copies.values():
        copy.wait_send()
    for group in grad_copies:
        for copy in group:
            copy.wait_send()


def fabric(sent, kept, key_total, value_total, owners, slots, places, capacity, dp_count, tensor_count):
    count = dp_count * tensor_count
    heads, quarter = owners.shape
    height = kept.shape[0]
    width = height // heads
    stages, spread = dp_count.bit_length() - 1, tensor_count.bit_length() - 1
    depth, columns = key_total.shape[0] // dp_count, key_total.shape[1]
    split = (dp_count // 2, 2, depth, columns)
    f32 = jnp.float32
    halved = [pltpu.VMEM((2, dp_count >> (s + 1), depth, columns), f32) for s in range(stages)]
    recv = jax.ShapeDtypeStruct((count, width + heads, capacity), f32)
    grad = jax.ShapeDtypeStruct((depth, columns), f32)
    space = pl.BlockSpec(memory_space=pl.ANY)
    vmem = pl.BlockSpec(memory_space=pltpu.VMEM)
    dma = pltpu.SemaphoreType.DMA
    return pl.pallas_call(
        functools.partial(fabric_kernel, dp_count, tensor_count, width),
        out_shape=(recv, grad, grad),
        in_specs=[space] * 4 + [vmem] * 3,
        out_specs=(space, vmem, vmem),
        scratch_shapes=[
            pltpu.VMEM((height, quarter), f32),
            pltpu.VMEM(kept.shape, f32),
            pltpu.VMEM(recv.shape, f32),
            pltpu.VMEM((2, dp_count // 2, depth, columns), f32),
        ]
        + halved
        + halved
        + [pltpu.VMEM((height, kept.shape[1] >> s), f32) for s in range(spread)]
        + [pltpu.VMEM((height, kept.shape[1] >> s), f32) for s in range(1, spread)]
        + [
            dma((4,)),
            dma((stages, dp_count // 2, 2)),
            dma((stages, dp_count // 2, 2)),
            dma((spread, 4)),
            dma((spread, 4)),
            dma((count,)),
            dma((count,)),
        ],
        compiler_params=pltpu.CompilerParams(
            collective_id=1, has_side_effects=True, vmem_limit_bytes=60_000_000
        ),
        cost_estimate=pl.CostEstimate(
            flops=80_000_000_000, bytes_accessed=20_000_000, transcendentals=0
        ),
        name="fabric",
    )(sent, kept, key_total.reshape(split), value_total.reshape(split), owners, slots, places)


def update_kernel(group, recv_ref, table_ref, sums_ref, new_table_ref, new_sums_ref, total):
    width, rows = table_ref.shape
    count, _, capacity = recv_ref.shape
    total[...] = jnp.zeros_like(total)

    def step(i, carry):
        picks, highs, lows = [], [], []
        for j in range(group):
            block = recv_ref[i * group + j]
            tag = jnp.sum(block[width:, :], axis=0, keepdims=True).astype(jnp.int32) - 1
            ids = lax.broadcasted_iota(jnp.int32, (rows, capacity), 0)
            picks.append((ids == tag).astype(jnp.float32).astype(jnp.bfloat16))
            high, low = halves(block[:width, :])
            highs.append(high)
            lows.append(low)
        pick = jnp.concatenate(picks, axis=1) if group > 1 else picks[0]
        high = jnp.concatenate(highs, axis=1) if group > 1 else highs[0]
        low = jnp.concatenate(lows, axis=1) if group > 1 else lows[0]
        total[...] += lax.dot_general(
            high, pick, OVER_FEATURES, preferred_element_type=jnp.float32
        ) + lax.dot_general(low, pick, OVER_FEATURES, preferred_element_type=jnp.float32)
        return carry

    lax.fori_loop(0, count // group, step, 0)
    row_sum = total[...]
    new_sum = sums_ref[...] + row_sum * row_sum
    new_sums_ref[...] = new_sum
    new_table_ref[...] = table_ref[...] - LEARN_RATE * row_sum / (jnp.sqrt(new_sum) + EPSILON)


def update_rows(recv, table, sums):
    group = 4 if recv.shape[2] % 128 == 0 and recv.shape[0] % 4 == 0 else 1
    return pl.pallas_call(
        functools.partial(update_kernel, group),
        out_shape=(jax.ShapeDtypeStruct(table.shape, jnp.float32),) * 2,
        in_specs=[pl.BlockSpec(memory_space=pltpu.VMEM)] * 3,
        out_specs=(pl.BlockSpec(memory_space=pltpu.VMEM),) * 2,
        scratch_shapes=[pltpu.VMEM(table.shape, jnp.float32)],
        cost_estimate=pl.CostEstimate(
            flops=6_000_000_000, bytes_accessed=5_000_000, transcendentals=0
        ),
        name="update_rows",
    )(recv, table, sums)


def body(hidden, out_grad, memory, w_key, w_value, row_owner, row_slot, mem_table, adagrad_sum):
    dp_count, tensor_count = lax.axis_size("dp"), lax.axis_size("tensor")
    owner_count = dp_count * tensor_count
    tokens = memory.shape[0]
    quarter = tokens // tensor_count
    features = w_key.shape[1] * tensor_count
    heads = row_owner.shape[1]
    scale_root = jnp.sqrt(jnp.asarray(features, jnp.float32))
    me = lax.axis_index("tensor")

    spread = tensor_count.bit_length() - 1
    firsts, extent = [], tokens
    for bit in range(spread):
        extent //= 2
        firsts.append(lax.rem(lax.div(me, 1 << bit), 2))
    first_row, extent = 0, tokens
    for mine in firsts:
        extent //= 2
        first_row = first_row + mine * extent
    owners = lax.dynamic_slice_in_dim(row_owner, first_row, quarter, 0).T
    slots = lax.dynamic_slice_in_dim(row_slot, first_row, quarter, 0).T.astype(jnp.float32)
    owner_ids = jnp.arange(owner_count, dtype=jnp.int32)
    hits = jnp.any(owners[None, :, :] == owner_ids[:, None, None], axis=1)
    token_ids = jnp.arange(quarter, dtype=jnp.int32)
    earlier = (token_ids[:, None] < token_ids[None, :]).astype(jnp.bfloat16)
    before = jnp.dot(hits.astype(jnp.bfloat16), earlier, preferred_element_type=jnp.float32)
    places = jnp.where(hits, before.astype(jnp.int32), -1)
    capacity = max(2, 2 * quarter * heads // owner_count)

    proj_key = jnp.dot(memory, w_key, preferred_element_type=jnp.float32)
    proj_value = jnp.dot(memory, w_value, preferred_element_type=jnp.float32)
    part_score = jnp.sum(hidden.astype(jnp.float32) * proj_key, axis=1)
    part_gate = jnp.sum(out_grad.astype(jnp.float32) * proj_value, axis=1)
    parts = jnp.stack([part_score, part_gate]).reshape(2, tokens // 128, 128)
    scores, gate_grad = sum_over_tensor(parts, tensor_count).reshape(2, tokens)
    gate_value = jax.nn.sigmoid(scores / scale_root)
    score_grad = gate_grad * gate_value * (1.0 - gate_value) / scale_root
    value_grad = (gate_value[:, None] * out_grad.astype(jnp.float32)).astype(jnp.bfloat16)
    key_grad = (score_grad[:, None] * hidden.astype(jnp.float32)).astype(jnp.bfloat16)
    hidden_grad = (score_grad[:, None] * proj_key).astype(jnp.bfloat16)

    def memory_grad_of(first, extent):
        value_part = lax.dynamic_slice_in_dim(value_grad, first, extent, 0)
        key_part = lax.dynamic_slice_in_dim(key_grad, first, extent, 0)
        return lax.dot_general(
            w_value, value_part, OVER_FEATURES, preferred_element_type=jnp.float32
        ) + lax.dot_general(w_key, key_part, OVER_FEATURES, preferred_element_type=jnp.float32)

    half = tokens // 2
    sent = memory_grad_of((1 - firsts[0]) * half, half)
    kept = memory_grad_of(firsts[0] * half, half)
    over_tokens = (((0,), (0,)), ((), ()))
    key_total = lax.dot_general(memory, key_grad, over_tokens, preferred_element_type=jnp.float32)
    value_total = lax.dot_general(
        memory, value_grad, over_tokens, preferred_element_type=jnp.float32
    )
    recv, key_weight_grad, value_weight_grad = fabric(
        sent, kept, key_total, value_total, owners, slots, places, capacity, dp_count, tensor_count
    )
    new_table, new_sum = update_rows(recv, mem_table.T, adagrad_sum.T)
    new_table, new_sum = new_table.T, new_sum.T
    return (hidden_grad, key_weight_grad, value_weight_grad, new_table, new_sum)


def solution(mesh):
    return jax.shard_map(
        body,
        mesh=mesh,
        in_specs=(
            P("dp", "tensor"),
            P("dp", "tensor"),
            P("dp", None),
            P(None, "tensor"),
            P(None, "tensor"),
            P("dp", None),
            P("dp", None),
            P(("dp", "tensor"), None),
            P(("dp", "tensor"), None),
        ),
        out_specs=(
            P("dp", "tensor"),
            P("dp", "tensor"),
            P("dp", "tensor"),
            P(("dp", "tensor"), None),
            P(("dp", "tensor"), None),
        ),
        check_vma=False,
    )
```
